32 devices in a mesh: aa: 8 (over z, y), ba: 4 (over x, core).
Axes of the slice: x: 2, y: 2, z: 4, core: 2. Of those that a mesh axis runs over, the one named last changes fastest.
Arguments:
- tokens: bfloat16 [4096, 8192], P('aa', 'ba'), may hold values from -6 to 6
- request_adapter_index: int32 [4096, 1], P('aa'), may hold values from 0 to 127; in each aligned block of 512 rows (0 to 511, 512 to 1023, ...) at most 8 rows name the same one
- key_weight: bfloat16 [8192, 1024], P('ba'), may hold values from -0.0625 to 0.0625
- value_weight: bfloat16 [8192, 1024], P('ba'), may hold values from -0.0625 to 0.0625
- adapter_down_weight: bfloat16 [128, 32, 8192], P('aa', None, 'ba'), may hold values from -0.0625 to 0.0625
- adapter_up_weight: bfloat16 [128, 2, 16, 1024], P('aa'), may hold values from -1.5 to 1.5
Outputs:
- keys_out: bfloat16 [4096, 1024], P('aa', 'ba')
- values_out: bfloat16 [4096, 1024], P('aa', 'ba')
The draws below stay inside these ranges and needn't reach their ends.
Inputs may be any that keep to these rules, and one draw needn't show every extreme that they name: `request_adapter_index`: among the 512 rows of one device no adapter is named more than 8 times, a bound that some block reaches.
All inputs are finite; a program needn't handle non-finite values.
Results may differ from the reference program's by a relative error of at most 0.001.
Values may be sent and summed in bfloat16 or wider, within the bound.
No kernel may reach another device: no remote copies, remote signals or barrier semaphores. Data moves between devices by JAX's collectives and lax.ppermute only.
A program may use at most 128 MiB of HBM per device.

```python
import math
import jax
import jax.numpy as jnp
import numpy as np
from jax import lax

MODEL_WIDTH = 8192
KEY_VALUE_WIDTH = 1024
ADAPTER_RANK = 16
ADAPTER_COUNT = 128
TOK_DEV = 512
TOKENS = 4096
ACAP = 8


def block_scale(stream_key, dims, split, least, high):
    gain, own = 1.0, jax.random.fold_in(stream_key, 6)
    for axis_at, blocks in split:
        heights = jnp.exp(jax.random.uniform(jax.random.fold_in(own, axis_at), (blocks,), jnp.float32, least / len(split), high / len(split)))
        gain = gain * jnp.repeat(heights, dims[axis_at] // blocks).reshape([-1 if axis == axis_at else 1 for axis in range(len(dims))])
    return gain


def shared_out(stream_key, own, number, rows, count, top, limit, lean):
    sequence = jax.random.permutation(stream_key, count)
    heavy_load, usual = portions_of(count, rows * top, limit, lean, True), portions_of(count, rows * top, limit, lean, False)
    places = jnp.arange(count)

    def named(tallies, offset_by):
        used = int((tallies > 0).sum())
        fixed = max(1, used // 4)
        shifted = fixed + (places - fixed + offset_by * (used - fixed)) % max(1, count - fixed)
        return jnp.zeros((count,), jnp.int32).at[sequence[jnp.where(places < fixed, places, shifted)]].set(jnp.asarray(tallies, jnp.int32))

    tallies = jnp.where(number % 4 == 0, named(heavy_load, number // 4), named(usual, number - number // 4 - 1))
    mixed = jax.random.permutation(jax.random.fold_in(own, 3), count)
    giver, sink = mixed[0:count // 2 * 2:2], mixed[1:count // 2 * 2:2]
    room = jnp.minimum(tallies[giver] - 1, limit - tallies[sink]) // 2
    room = jnp.where((giver == sequence[0]) | (sink == sequence[0]) | (tallies[sink] == 0), 0, jnp.maximum(room, 0))
    shifted = jax.random.randint(jax.random.fold_in(own, 4), (count // 2,), 0, 1 << 20) % (room + 1)
    tallies = tallies.at[giver].add(-shifted).at[sink].add(shifted)
    labels = jnp.searchsorted(jnp.cumsum(tallies), jnp.arange(rows * top), side="right").astype(jnp.int32)
    listing = labels.reshape(top, rows).T
    listing = listing[jax.random.permutation(jax.random.fold_in(own, 1), rows)]
    offset_by = jax.random.randint(jax.random.fold_in(own, 2), (rows, 1), 0, top)
    return jnp.take_along_axis(listing, (jnp.arange(top)[None, :] + offset_by) % top, axis=1)


def portions_of(number_of, total, reach, slope, full):
    portions = [(1 << 20) // math.isqrt(standing ** slope) + 1 for standing in range(1, number_of + 1)]
    largest = reach if full else min(reach, max(-(-total // number_of), total * portions[0] // sum(portions)))
    least = 1 if total - largest >= number_of - 1 else 0
    counts, rest = [largest] + [least] * (number_of - 1), total - largest - least * (number_of - 1)
    while rest > 0:
        movable = [i for i in range(1, number_of) if counts[i] < largest] or [i for i in range(1, number_of) if counts[i] < reach]
        whole, remaining = sum([portions[i] for i in movable]), rest
        for i in movable:
            addition = min(reach - counts[i], max(1, remaining * portions[i] // whole), rest)
            counts[i] = counts[i] + addition
            rest = rest - addition
    return np.array(counts)


def noise(own_key, extent, deviation, limit, cuts=(), kind=jnp.bfloat16):
    entries = jax.random.normal(own_key, extent, jnp.float32) * deviation
    if len(cuts) > 0:
        entries = block_scale(own_key, extent, cuts, -0.22, 0.18) * entries
    return jnp.clip(entries, min=-limit, max=limit).astype(kind)


def setup_inputs(seed: int = 0) -> dict:
    splits = jax.random.split(jax.random.key(seed), 7)
    tokens = noise(splits[0], (TOKENS, MODEL_WIDTH), 1.0, 6.0, ((0, 8), (1, 4)))
    request_adapter_index_keys = jax.random.split(jax.random.fold_in(splits[1], 1), TOKENS // TOK_DEV)
    request_adapter_index_turns = jax.random.permutation(jax.random.fold_in(splits[1], 3), TOKENS // TOK_DEV)
    request_adapter_index = jax.vmap(lambda own, number: shared_out(jax.random.fold_in(splits[1], 2), own, number, TOK_DEV, ADAPTER_COUNT, 1, ACAP, 2))(request_adapter_index_keys, request_adapter_index_turns).reshape((TOKENS, 1))
    key_weight = noise(splits[2], (MODEL_WIDTH, KEY_VALUE_WIDTH), MODEL_WIDTH ** -0.5, 0.0625, ((0, 4),))
    value_weight = noise(splits[3], (MODEL_WIDTH, KEY_VALUE_WIDTH), MODEL_WIDTH ** -0.5, 0.0625, ((0, 4),))
    adapter_down_weight = noise(splits[4], (ADAPTER_COUNT, 2 * ADAPTER_RANK, MODEL_WIDTH), MODEL_WIDTH ** -0.5, 0.0625, ((0, 8), (2, 4)))
    adapter_up_weight = noise(splits[5], (ADAPTER_COUNT, 2, ADAPTER_RANK, KEY_VALUE_WIDTH), ADAPTER_RANK ** -0.5, 1.5, ((0, 8),))
    return {"tokens": tokens, "request_adapter_index": request_adapter_index, "key_weight": key_weight, "value_weight": value_weight, "adapter_down_weight": adapter_down_weight, "adapter_up_weight": adapter_up_weight}


def reference(tokens, request_adapter_index, key_weight, value_weight, adapter_down_weight, adapter_up_weight):
    base_key = jnp.dot(tokens, key_weight, preferred_element_type=jnp.float32)
    base_value = jnp.dot(tokens, value_weight, preferred_element_type=jnp.float32)
    height = math.gcd(TOKENS, 64)
    token_blocks = tokens.reshape(TOKENS // height, height, MODEL_WIDTH)
    adapter_blocks = request_adapter_index.reshape(TOKENS // height, height)

    def one_block(pair):
        rows, selected_adapter = pair
        down_weight_rows = adapter_down_weight[selected_adapter].astype(jnp.float32)
        up_weight_rows = adapter_up_weight[selected_adapter].astype(jnp.float32)
        rank_sum = jnp.einsum("td,tjd->tj", rows.astype(jnp.float32), down_weight_rows, precision=lax.Precision.HIGHEST)
        key_change = jnp.einsum("tr,trc->tc", rank_sum[:, :ADAPTER_RANK], up_weight_rows[:, 0], precision=lax.Precision.HIGHEST)
        value_change = jnp.einsum("tr,trc->tc", rank_sum[:, ADAPTER_RANK:], up_weight_rows[:, 1], precision=lax.Precision.HIGHEST)
        return key_change, value_change

    key_change, value_change = lax.map(one_block, (token_blocks, adapter_blocks))
    keys_out = (base_key + key_change.reshape(TOKENS, KEY_VALUE_WIDTH)).astype(jnp.bfloat16)
    values_out = (base_value + value_change.reshape(TOKENS, KEY_VALUE_WIDTH)).astype(jnp.bfloat16)
    return keys_out, values_out
```

```python
import functools

import jax
import jax.numpy as jnp
from jax import lax
from jax.experimental import pallas as pl
from jax.experimental.pallas import tpu as pltpu
from jax.sharding import PartitionSpec as P


F32 = jnp.float32
BF16 = jnp.bfloat16
LANES = 128
VMEM_BYTES = 48 * 1024 * 1024


def round_up(x, m):
    return -(-x // m) * m


def params():
    return pltpu.CompilerParams(vmem_limit_bytes=VMEM_BYTES)


def smem():
    return pl.BlockSpec(memory_space=pltpu.SMEM)


def vmem():
    return pl.BlockSpec(memory_space=pltpu.VMEM)


def routing(idx_col, homes, resident):
    rows = idx_col.shape[0]
    i0 = lax.broadcasted_iota(jnp.int32, (rows, rows), 0)
    i1 = lax.broadcasted_iota(jnp.int32, (rows, rows), 1)
    col = idx_col.astype(F32)
    row = jnp.sum(jnp.where(i0 == i1, col, 0.0), axis=0, keepdims=True)

    def home(v):
        h = jnp.zeros_like(v)
        for k in range(1, homes):
            h = h + jnp.where(v >= float(k * resident), 1.0, 0.0)
        return h

    home_row, home_col = home(row), home(col)
    same = (home_col == home_row) & (i0 < i1)
    pos_row = jnp.sum(jnp.where(same, 1.0, 0.0), axis=0, keepdims=True)
    return home_row, row - float(resident) * home_row, pos_row


def one_hot(home_row, rel_row, home, usable, height):
    hit = (home_row == home) & (rel_row >= 0.0) & (rel_row < float(usable))
    key = jnp.where(hit, rel_row, -1.0)
    slots = lax.broadcasted_iota(jnp.int32, (height, home_row.shape[1]), 0).astype(F32)
    return jnp.where(slots == key, 1.0, 0.0).astype(BF16)


def gather_body(scal, idx, tok, *outs, homes, resident, dists, chunk):
    rows, width = tok.shape
    home_row, local_row, pos_row = routing(idx[...], homes, resident)
    usable = chunk - 1
    rel = pos_row - scal[1].astype(F32)
    rounds = jnp.floor((jnp.max(pos_row, axis=1, keepdims=True) + 0.5) / float(usable)) + 1.0
    hots = [one_hot(home_row, rel, (scal[0] ^ d).astype(F32), usable, LANES) for d in dists]
    picked = jnp.dot(
        jnp.concatenate([h[:chunk] for h in hots], axis=0), tok[...], preferred_element_type=F32
    )
    local8 = jnp.broadcast_to(local_row, (8, rows)).astype(BF16)
    last = lax.broadcasted_iota(jnp.int32, (16, 2 * LANES), 0) == 15
    for n, out in enumerate(outs):
        block = picked[n * chunk : (n + 1) * chunk]
        out[...] = block.astype(BF16)
        ids = lax.dot_general(local8, hots[n], (((1,), (1,)), ((), ())), preferred_element_type=F32)
        meta = jnp.concatenate([ids[:1], jnp.broadcast_to(rounds, (1, LANES))], axis=1)
        tail = jnp.where(last, meta, block[chunk - 16 :, : 2 * LANES])
        out[chunk - 16 :, : 2 * LANES] = tail.astype(BF16)


def gather(tokens, index, me, offset, dists, homes, resident, chunk):
    width = tokens.shape[1]
    return pl.pallas_call(
        functools.partial(
            gather_body, homes=homes, resident=resident, dists=dists, chunk=chunk
        ),
        in_specs=[smem(), vmem(), vmem()],
        out_specs=[vmem() for _ in dists],
        out_shape=[jax.ShapeDtypeStruct((chunk, width), BF16) for _ in dists],
        compiler_params=params(),
        name=f"gather_{dists[0]}",
    )(jnp.stack([me, offset]), index, tokens)


def rank_body(scal, down, *refs, homes, resident, chunk):
    chunks, out, rounds_out = refs[:homes], refs[homes], refs[homes + 1]
    two_rank = down.shape[0] // resident
    x = jnp.concatenate([c[...] for c in chunks], axis=0)
    full = lax.dot_general(x, down[...], (((1,), (1,)), ((), ())), preferred_element_type=F32)
    eye = lax.broadcasted_iota(jnp.int32, (chunk, LANES), 0) == lax.broadcasted_iota(
        jnp.int32, (chunk, LANES), 1
    )
    columns = resident * two_rank
    owner = (lax.broadcasted_iota(jnp.int32, (1, columns), 1) // two_rank).astype(F32)
    most = jnp.zeros((1, LANES), F32)
    for k in range(homes):
        meta = chunks[k][chunk - 16 :, : 2 * LANES].astype(F32)[15:16]
        most = jnp.maximum(most, meta[:, LANES:])
        ids = jnp.sum(jnp.where(eye, meta[:, :LANES], 0.0), axis=1, keepdims=True)
        mine = jnp.where(owner == ids, full[k * chunk : (k + 1) * chunk], 0.0)
        acc = mine[:, :LANES]
        for c in range(LANES, columns, LANES):
            acc = acc + mine[:, c : c + LANES]
        shift = LANES // 2
        while shift >= two_rank:
            acc = acc + pltpu.roll(acc, shift, 1)
            shift //= 2
        if chunk < LANES:
            acc = jnp.concatenate([acc, jnp.zeros((LANES - chunk, LANES), F32)], axis=0)
        out[scal[0] ^ k] = acc.T[:two_rank]
    rounds_out[...] = most.astype(jnp.int32)


def rank(chunks, down, me, homes, resident, chunk):
    two_rank = down.shape[0] // resident
    return pl.pallas_call(
        functools.partial(rank_body, homes=homes, resident=resident, chunk=chunk),
        in_specs=[smem(), vmem()] + [vmem() for _ in chunks],
        out_specs=[vmem(), vmem()],
        out_shape=[
            jax.ShapeDtypeStruct((homes, two_rank, LANES), F32),
            jax.ShapeDtypeStruct((1, LANES), jnp.int32),
        ],
        compiler_params=params(),
        name="rank",
    )(me[None], down, *chunks)


def split3(x):
    hi = x.astype(BF16)
    rest = x - hi.astype(F32)
    mid = rest.astype(BF16)
    return hi, mid, (rest - mid.astype(F32)).astype(BF16)


def unpermute_body(scal, idx, ret, out, *, homes, resident, chunk):
    home_row, _, pos_row = routing(idx[...], homes, resident)
    rel = pos_row - scal[0].astype(F32)
    hots = jnp.concatenate(
        [one_hot(home_row, rel, float(h), chunk - 1, LANES) for h in range(homes)], axis=0
    )
    values = jnp.concatenate([ret[h] for h in range(homes)], axis=1)
    two_rank = values.shape[0]
    pieces = jnp.concatenate(split3(values), axis=0)
    res = jnp.dot(pieces, hots, preferred_element_type=F32)
    out[...] = res[:two_rank] + (res[two_rank : 2 * two_rank] + res[2 * two_rank :])


def unpermute(index, returned, offset, homes, resident, chunk):
    return pl.pallas_call(
        functools.partial(unpermute_body, homes=homes, resident=resident, chunk=chunk),
        in_specs=[smem(), vmem(), vmem()],
        out_specs=vmem(),
        out_shape=jax.ShapeDtypeStruct((returned.shape[1], index.shape[0]), F32),
        compiler_params=params(),
        name="unpermute",
    )(offset[None], index, returned)


def base_body(order, tok, key, value, out):
    x = tok[...]
    out[0, :, : key.shape[1]] = jnp.dot(x, key[...], preferred_element_type=F32)
    out[0, :, key.shape[1] :] = jnp.dot(x, value[...], preferred_element_type=F32)


def base(tokens, key_weight, value_weight, owners, kv_local, name):
    rows, width = tokens.shape
    count = owners.shape[0]
    weight = pl.BlockSpec((width, kv_local), lambda s, o: (0, o[s]))
    return pl.pallas_call(
        base_body,
        grid_spec=pltpu.PrefetchScalarGridSpec(
            num_scalar_prefetch=1,
            grid=(count,),
            in_specs=[pl.BlockSpec((rows, width), lambda s, o: (0, 0)), weight, weight],
            out_specs=pl.BlockSpec((1, rows, 2 * kv_local), lambda s, o: (s, 0, 0)),
        ),
        out_shape=jax.ShapeDtypeStruct((count, rows, 2 * kv_local), F32),
        compiler_params=params(),
        name=name,
    )(owners, tokens, key_weight, value_weight)


def final_body(blocks_home, idx, *refs, ranks, bases, resident):
    rank_refs = refs[:ranks]
    base_refs = refs[ranks : ranks + bases]
    ups = refs[ranks + bases : -2]
    keys, values = refs[-2:]
    total = rank_refs[0][...]
    for r in rank_refs[1:]:
        total = total + r[...]
    kv_local = keys.shape[1]
    half = total.shape[0] // 2
    columns = resident * half
    cols = total.T
    fill = (
        lax.broadcasted_iota(jnp.int32, (half, columns), 1) % half
        == lax.broadcasted_iota(jnp.int32, (half, columns), 0)
    )
    fill = jnp.where(fill, 1.0, 0.0).astype(BF16)
    spread = []
    for part in (cols[:, :half], cols[:, half:]):
        hi = part.astype(BF16)
        lo = (part - hi.astype(F32)).astype(BF16)
        spread.append(
            [jnp.dot(p, fill, preferred_element_type=F32).astype(BF16) for p in (hi, lo)]
        )
    owner = lax.broadcasted_iota(jnp.int32, (1, columns), 1) // half
    index = idx[...]
    for side, out in enumerate((keys, values)):
        acc = base_refs[0][:, side * kv_local : (side + 1) * kv_local]
        for b in base_refs[1:]:
            acc = acc + b[:, side * kv_local : (side + 1) * kv_local]
        for n, up in enumerate(ups):
            mine = index == owner + blocks_home[n] * resident
            weight = up[:, side].reshape(columns, kv_local)
            for piece in spread[side]:
                lhs = jnp.where(mine, piece, jnp.zeros_like(piece))
                acc = acc + jnp.dot(lhs, weight, preferred_element_type=F32)
        out[...] = acc.astype(BF16)


def final(index, blocks_home, rank_parts, base_parts, ups):
    rows = index.shape[0]
    kv_local = ups[0].shape[-1]
    args = (index, *rank_parts, *base_parts, *ups)
    return pl.pallas_call(
        functools.partial(
            final_body, ranks=len(rank_parts), bases=len(base_parts), resident=ups[0].shape[0]
        ),
        in_specs=[smem()] + [vmem() for _ in args],
        out_specs=[vmem(), vmem()],
        out_shape=[jax.ShapeDtypeStruct((rows, kv_local), BF16)] * 2,
        compiler_params=params(),
        name="final",
    )(blocks_home, *args)


def xor_pairs(size, dist):
    return [(i, i ^ dist) for i in range(size)]


def on_device(
    tokens, request_adapter_index, key_weight, value_weight, adapter_down_weight, adapter_up_weight
):
    homes = lax.axis_size("aa")
    splits = lax.axis_size("ba")
    rows, width = tokens.shape
    resident, two_rank, _ = adapter_down_weight.shape
    kv_local = key_weight.shape[1] // splits
    me = lax.axis_index("aa")
    mb = lax.axis_index("ba")
    down = adapter_down_weight.reshape(resident * two_rank, width)
    chunk = min(LANES, round_up(rows * 5 // (4 * homes), 16))
    near = tuple(range(homes // 2))
    far = tuple(range(homes // 2, homes))

    def exchange(offset):
        chunks = {}
        for dists in (far, near):
            picked = gather(
                tokens, request_adapter_index, me, offset, dists, homes, resident, chunk
            )
            for d, p in zip(dists, picked):
                chunks[d] = p if d == 0 else lax.ppermute(p, "aa", xor_pairs(homes, d))
        parts, rounds = rank(
            [chunks[d] for d in range(homes)], down, me, homes, resident, chunk
        )
        returned = lax.all_to_all(parts, "aa", split_axis=0, concat_axis=0, tiled=True)
        part = unpermute(request_adapter_index, returned, offset, homes, resident, chunk)
        return part, rounds[0, 0]

    part, rounds = exchange(jnp.int32(0))

    blocks = {}
    low = splits // 2
    sending = jnp.stack([mb ^ (2 * s + 1) for s in range(low)])
    keeping = jnp.stack([mb ^ (2 * s) for s in range(low)])
    sent = base(tokens, key_weight, value_weight, sending, kv_local, "base_send")
    kept = base(tokens, key_weight, value_weight, keeping, kv_local, "base_keep")
    got = lax.ppermute(sent, "ba", xor_pairs(splits, 1))
    base_parts = {2 * s: [kept[s], got[s]] for s in range(low)}
    bit = 2
    while bit < splits:
        arrived = {}
        for d in [d for d in base_parts if d & bit]:
            piece = functools.reduce(jnp.add, base_parts.pop(d))
            arrived[d ^ bit] = lax.ppermute(piece, "ba", xor_pairs(splits, bit))
        for d, piece in arrived.items():
            base_parts[d] = base_parts[d] + [piece]
        bit *= 2
    base_parts = base_parts[0]

    pair = 2 if homes % 2 == 0 else 1
    line = homes // pair
    own = lax.dynamic_slice_in_dim(adapter_up_weight, mb * kv_local, kv_local, 3)
    right = [(i, i + pair) for i in range(homes - pair)]
    left = [(j, i) for i, j in right]
    from_left, from_right = {0: own}, {0: own}
    for s in range(1, line):
        from_left[s] = lax.ppermute(from_left[s - 1], "aa", right)
        from_right[s] = lax.ppermute(from_right[s - 1], "aa", left)
    ups = [own] + [from_left[s] + from_right[line - s] for s in range(1, line)]
    place = me // pair
    ups_home = [((place - s) % line) * pair + me % pair for s in range(line)]
    if pair == 2:
        ups_home = ups_home + [h ^ 1 for h in ups_home]
        ups = ups + [lax.ppermute(u, "aa", xor_pairs(homes, 1)) for u in ups]

    usable = chunk - 1
    part = lax.while_loop(
        lambda c: c[0] < rounds,
        lambda c: (c[0] + 1, c[1] + exchange(c[0] * usable)[0]),
        (jnp.int32(1), part),
    )[1]
    rank_parts = [part] + [
        lax.ppermute(part, "ba", xor_pairs(splits, d)) for d in range(1, splits)
    ]
    return tuple(
        final(request_adapter_index, jnp.stack(ups_home), rank_parts, base_parts, ups)
    )


def solution(mesh):
    return jax.shard_map(
        on_device,
        mesh=mesh,
        in_specs=(
            P("aa", "ba"),
            P("aa", None),
            P("ba", None),
            P("ba", None),
            P("aa", None, "ba"),
            P("aa", None, None, None),
        ),
        out_specs=(P("aa", "ba"), P("aa", "ba")),
        check_vma=False,
    )
```
